32 devices in a mesh: tm: 16 (over z, y, x), state: 2 (over core).
Axes of the slice: x: 2, y: 2, z: 4, core: 2. Of those that a mesh axis runs over, the one named last changes fastest.
Arguments:
- symbols: int32 [8], P('state'), may hold values from 0 to 255
- emission: float32 [8192, 256], P('tm'), may hold values from 0.2 to 5
- decay: float32 [2, 8192], P('state', 'tm'), may hold values from 0.05 to 1
- left_factor: float32 [2, 64, 8192], P('state', None, 'tm'), may hold values from 0.1 to 3
- right_factor: float32 [2, 64, 8192], P('state', None, 'tm'), may hold values from 0.001 to 0.03
- initial: float32 [8192], P('tm'), may hold values from 0.1 to 10
Outputs:
- filtered: float32 [8, 8192], P('state', 'tm')
- log_scale: float32 [8], P('state')
The draws below stay inside these ranges and needn't reach their ends.
All inputs are finite; a program needn't handle non-finite values.
Results may differ from the reference program's by a relative error of at most 0.00011.
Values sent between devices are 32-bit elements; how exact they have to be, the bound alone decides.
A program may use at most 64 MiB of HBM per device.

```python
import math
import jax
import jax.numpy as jnp
from jax import lax

S = 8192
R = 64
NSYM = 256
F_DEV = 4
SPANS = 2
FRAMES = 8
N_STATE = 2


def plant(entries, own_key, least, top_value):
    dims = entries.shape
    index_at = [jax.random.randint(jax.random.fold_in(own_key, axis), (), 0, dims[axis]) for axis in range(len(dims))]
    entries = entries.at[tuple(index_at)].set(least)
    longest = dims.index(max(dims))
    index_at[longest] = (index_at[longest] + 1) % dims[longest]
    return entries.at[tuple(index_at)].set(top_value)


def level_of(rng, shape, pieces, least, largest):
    loudness, own = 1.0, jax.random.fold_in(rng, 6)
    for position, parts in pieces:
        steps = jnp.exp(jax.random.uniform(jax.random.fold_in(own, position), (parts,), jnp.float32, least / len(pieces), largest / len(pieces)))
        loudness = loudness * jnp.repeat(steps, shape[position] // parts).reshape([-1 if axis == position else 1 for axis in range(len(shape))])
    return loudness


def setup_inputs(seed: int = 0) -> dict:
    keys = jax.random.split(jax.random.key(seed), 7)
    symbols = plant(jax.random.randint(keys[0], (FRAMES,), 0, NSYM), jax.random.fold_in(keys[0], 1), 0, NSYM - 1).astype(jnp.int32)
    emission = jnp.clip(jnp.exp(math.log(5.0) - 3.218876 * jax.random.uniform(keys[1], (S, NSYM), jnp.float32) ** level_of(keys[1], (S, NSYM), ((0, 16),), -0.2, 0.2)), 0.2, 5.0)
    decay = jnp.clip(jnp.exp(math.log(1.0) - 2.9957323 * jax.random.uniform(keys[2], (SPANS, S), jnp.float32) ** level_of(keys[2], (SPANS, S), ((0, 2), (1, 16)), -0.2, 0.2)), 0.05, 1.0)
    left_factor = jnp.clip(jnp.exp(math.log(3.0) - 3.4011974 * jax.random.uniform(keys[3], (SPANS, R, S), jnp.float32) ** level_of(keys[3], (SPANS, R, S), ((0, 2), (2, 16)), -0.2, 0.2)), 0.1, 3.0)
    right_factor = jnp.clip(jnp.exp(math.log(0.03) - 3.4011973 * jax.random.uniform(keys[4], (SPANS, R, S), jnp.float32) ** level_of(keys[4], (SPANS, R, S), ((0, 2), (2, 16)), -0.2, 0.2)), 0.001, 0.03)
    initial = jnp.clip(jnp.exp(math.log(10.0) - 4.6051702 * jax.random.uniform(keys[5], (S,), jnp.float32) ** level_of(keys[5], (S,), ((0, 16),), -0.2, 0.2)), 0.1, 10.0)
    return {"symbols": symbols, "emission": emission, "decay": decay, "left_factor": left_factor, "right_factor": right_factor, "initial": initial}


PRECISE = lax.Precision.HIGHEST


def reference(symbols, emission, decay, left_factor, right_factor, initial):
    belief_init = initial / jnp.mean(initial)

    def block(belief, inputs):
        symbol_row, decay_row, left_rows, right_rows = inputs

        def frame(belief_now, symbol):
            emitted = lax.dynamic_index_in_dim(emission, symbol, 1, keepdims=False)
            mixture = jnp.dot(left_rows, belief_now, precision=PRECISE) / S
            unscaled = emitted * (decay_row * belief_now + jnp.dot(mixture, right_rows, precision=PRECISE))
            normal = jnp.sum(unscaled) / S
            belief_next = unscaled / normal
            return belief_next, (belief_next, jnp.log(normal))

        return lax.scan(frame, belief, symbol_row)

    closing, (beliefs, log_levels) = lax.scan(block, belief_init, (symbols.reshape(N_STATE, F_DEV), decay, left_factor, right_factor))
    return beliefs.reshape(N_STATE * F_DEV, S), log_levels.reshape(N_STATE * F_DEV)
```

```python
import functools

import jax
import jax.numpy as jnp
from jax import lax
from jax.experimental import pallas as pl
from jax.experimental.pallas import tpu as pltpu
from jax.sharding import PartitionSpec as P

F32 = jnp.float32
BF16 = jnp.bfloat16
ROWS = 8


def split(x):
    hi = x.astype(BF16)
    return hi, (x - hi.astype(F32)).astype(BF16)


def stacked(x):
    hi = x.astype(BF16).astype(F32)
    return jnp.concatenate([hi, x - hi], axis=0).astype(BF16)


def dot2(x, pieces, dims):
    both = stacked(x)
    total = sum(
        lax.dot_general(both, piece, (dims, ((), ())), preferred_element_type=F32)
        for piece in pieces
    )
    return total[: x.shape[0]] + total[x.shape[0] :]


ALONG = ((1,), (1,))
ACROSS = ((1,), (0,))


def kernel(
    tiles,
    spans,
    symbols,
    emission_hbm,
    decay_hbm,
    left_hbm,
    right_hbm,
    initial_hbm,
    beliefs_out,
    logs_out,
    emission,
    decay,
    left,
    right,
    entry,
    closing,
    side,
    kbuf,
    rbuf,
    gown,
    gbuf,
    kfull,
    pbuf,
    pall,
    load_sem,
    rs_send,
    rs_recv,
    ag_send,
    ag_recv,
    p_send,
    p_recv,
    pass_send,
    pass_recv,
):
    me = lax.axis_index("tm")
    span = lax.axis_index("state")
    frames = beliefs_out.shape[0]
    rank, cells = right.shape
    width = kfull.shape[1]
    share = rank // tiles
    states = cells * tiles
    pairs = [(t, s) for s in range(frames) for t in range(s + 1, frames)]
    sums = [(t, s) for s in range(frames) for t in range(s + 1, frames + 1)]

    barrier = pltpu.get_barrier_semaphore()
    peers = [lax.rem(me + k, tiles) for k in range(tiles)]
    for k in range(1, tiles):
        pl.semaphore_signal(barrier, inc=1, device_id={"tm": peers[k]})
    turns = sorted({1 % spans, (spans - 1) % spans} - {0})
    for k in turns:
        pl.semaphore_signal(barrier, inc=1, device_id={"state": lax.rem(span + k, spans)})

    loads = [
        pltpu.make_async_copy(src, dst, load_sem.at[i])
        for i, (src, dst) in enumerate(
            (
                (emission_hbm, emission),
                (decay_hbm, decay),
                (left_hbm.at[0], left),
                (right_hbm.at[0], right),
            )
        )
    ]
    for load in loads:
        load.start()

    @pl.when(span == 0)
    def _():
        copy = pltpu.make_async_copy(initial_hbm, entry, load_sem.at[4])
        copy.start()
        copy.wait()

    row_id = lax.broadcasted_iota(jnp.int32, (ROWS, emission.shape[1]), 0)
    column_id = lax.broadcasted_iota(jnp.int32, (ROWS, emission.shape[1]), 1)
    wanted = jnp.full(row_id.shape, -1, jnp.int32)
    for t in range(frames):
        wanted = jnp.where(row_id == t, symbols[t], wanted)
    onehot = jnp.where(wanted == column_id, 1.0, 0.0).astype(BF16)
    for load in loads:
        load.wait()
    emitted = sum(
        lax.dot_general(onehot, piece, (ALONG, ((), ())), preferred_element_type=F32)
        for piece in split(emission[...])
    )
    emit = [emitted[t : t + 1] for t in range(frames)]
    grow = [emit[t] * decay[...] for t in range(frames)]
    scaled = left[...] * (1.0 / states)
    scaled_pieces = split(scaled)

    def send_projection():
        row = entry[...]
        rows = [row]
        for t in range(frames):
            row = row * grow[t]
            rows.append(row)
        rows += [jnp.zeros_like(row)] * (ROWS - len(rows))
        reached = jnp.concatenate(rows, axis=0)
        pbuf[:, :rank] = dot2(reached, scaled_pieces, ALONG)
        pbuf[:, rank:] = jnp.broadcast_to(
            jnp.sum(reached, axis=1, keepdims=True), (ROWS, pbuf.shape[1] - rank)
        )
        for k in range(1, tiles):
            p_copy(k).start()

    def p_copy(k):
        return pltpu.make_async_remote_copy(
            pbuf, pall.at[k - 1], p_send.at[k - 1], p_recv.at[k - 1], device_id={"tm": peers[k]}
        )

    def rs_copy(k):
        return pltpu.make_async_remote_copy(
            kbuf.at[peers[k]],
            rbuf.at[k - 1],
            rs_send.at[k - 1],
            rs_recv.at[k - 1],
            device_id={"tm": peers[k]},
        )

    def ag_copy(k):
        return pltpu.make_async_remote_copy(
            gown, gbuf.at[me], ag_send.at[k - 1], ag_recv.at[k - 1], device_id={"tm": peers[k]}
        )

    def pass_copy():
        return pltpu.make_async_remote_copy(
            closing, entry, pass_send, pass_recv, device_id={"state": lax.rem(span + 1, spans)}
        )

    reach = {}
    for s in range(frames):
        weight = emit[s]
        reach[s + 1, s] = weight
        for t in range(s + 1, frames):
            weight = weight * grow[t]
            reach[t + 1, s] = weight
    for i, pair in enumerate(pairs):
        side[i * rank : (i + 1) * rank] = reach[pair] * scaled
    base = len(pairs) * rank
    side[base:] = jnp.zeros((width - base, cells), F32)
    for i, pair in enumerate(sums):
        side[base + i : base + i + 1] = reach[pair]

    coupling = dot2(right[...], split(side[...]), ALONG)
    for j in range(tiles):
        kbuf[j] = coupling[j * share : (j + 1) * share]

    pl.semaphore_wait(barrier, tiles - 1 + len(turns))

    @pl.when(span == 0)
    def _():
        send_projection()

    for k in range(1, tiles):
        rs_copy(k).start()
    total = kbuf[me]
    for k in range(1, tiles):
        rs_copy(k).wait_recv()
        total = total + rbuf[k - 1]
    gown[...] = total
    for k in range(1, tiles):
        ag_copy(k).start()
    gbuf[me] = total
    for k in range(1, tiles):
        ag_copy(k).wait_recv()
    for j in range(tiles):
        kfull[j * share : (j + 1) * share] = gbuf[j]
    matrices = {
        pair: split(kfull[:, i * rank : (i + 1) * rank]) for i, pair in enumerate(pairs)
    }
    sum_matrix = split(kfull[:, base:])

    @pl.when(span > 0)
    def _():
        pass_copy().wait_recv()
        send_projection()

    projected = pbuf[...]
    for k in range(1, tiles):
        p_copy(k).wait_recv()
        projected = projected + pall[k - 1]
    mix = projected[:, :rank]
    mix_row = lax.broadcasted_iota(jnp.int32, mix.shape, 0)
    mix = jnp.where(mix_row < frames, mix, 0.0)
    for s in range(frames - 1):
        for t in range(s + 1, frames):
            term = dot2(mix, matrices[t, s], ACROSS)[s : s + 1]
            mix = mix + jnp.where(mix_row == t, term, 0.0)
    lifted = dot2(mix, split(right[...]), ACROSS)
    belief = entry[...]
    kept = []
    for t in range(frames):
        belief = grow[t] * belief + emit[t] * lifted[t : t + 1]
        kept.append(belief)
    if spans > 1:
        closing[...] = belief

        @pl.when(span < spans - 1)
        def _():
            pass_copy().start()

    parts = dot2(mix, sum_matrix, ACROSS)
    part_row = lax.broadcasted_iota(jnp.int32, parts.shape, 0)
    part_column = lax.broadcasted_iota(jnp.int32, parts.shape, 1)
    mass = [projected[0:1, rank : rank + 1]]
    for t in range(1, frames + 1):
        hit = jnp.zeros(parts.shape, jnp.bool_)
        for i, (u, s) in enumerate(sums):
            if u == t:
                hit = hit | ((part_row == s) & (part_column == i))
        mass.append(
            projected[t : t + 1, rank : rank + 1]
            + jnp.sum(jnp.where(hit, parts, 0.0), keepdims=True)
        )
    lane = lax.broadcasted_iota(jnp.int32, logs_out.shape, 1)
    logs = jnp.zeros(logs_out.shape, F32)
    for t in range(frames):
        beliefs_out[t : t + 1] = kept[t] * (states / mass[t + 1])
        logs = jnp.where(lane == t, mass[t + 1] / mass[t], logs)
    logs_out[...] = jnp.log(jnp.where(lane < frames, logs, 1.0))

    for k in range(1, tiles):
        p_copy(k).wait_send()
        rs_copy(k).wait_send()
        ag_copy(k).wait_send()
    if spans > 1:

        @pl.when(span < spans - 1)
        def _():
            pass_copy().wait_send()


def solution(mesh):
    tiles, spans = mesh.shape["tm"], mesh.shape["state"]

    def per_device(symbols, emission, decay, left_factor, right_factor, initial):
        frames = symbols.shape[0]
        rank, cells = left_factor.shape[1:]
        pair_count = frames * (frames - 1) // 2
        sum_count = frames * (frames + 1) // 2
        width = -(-(pair_count * rank + sum_count) // 128) * 128
        share = rank // tiles
        vmem, dma = pltpu.VMEM, pltpu.SemaphoreType.DMA
        others = tiles - 1
        beliefs, logs = pl.pallas_call(
            functools.partial(kernel, tiles, spans),
            out_shape=(
                jax.ShapeDtypeStruct((frames, cells), F32),
                jax.ShapeDtypeStruct((1, 128), F32),
            ),
            in_specs=[pl.BlockSpec(memory_space=pltpu.SMEM)]
            + [pl.BlockSpec(memory_space=pl.ANY)] * 5,
            out_specs=(pl.BlockSpec(memory_space=vmem),) * 2,
            scratch_shapes=[
                vmem(emission.shape, F32),
                vmem(decay.shape, F32),
                vmem((rank, cells), F32),
                vmem((rank, cells), F32),
                vmem((1, cells), F32),
                vmem((1, cells), F32),
                vmem((width, cells), F32),
                vmem((tiles, share, width), F32),
                vmem((others, share, width), F32),
                vmem((share, width), F32),
                vmem((tiles, share, width), F32),
                vmem((rank, width), F32),
                vmem((ROWS, 128), F32),
                vmem((others, ROWS, 128), F32),
                dma((5,)),
                dma((others,)),
                dma((others,)),
                dma((others,)),
                dma((others,)),
                dma((others,)),
                dma((others,)),
                dma(()),
                dma(()),
            ],
            compiler_params=pltpu.CompilerParams(collective_id=0, has_side_effects=True),
        )(symbols, emission, decay, left_factor, right_factor, initial.reshape(1, cells))
        return beliefs, logs[0, :frames]

    return jax.shard_map(
        per_device,
        mesh=mesh,
        in_specs=(
            P("state"),
            P("tm", None),
            P("state", "tm"),
            P("state", None, "tm"),
            P("state", None, "tm"),
            P("tm"),
        ),
        out_specs=(P("state", "tm"), P("state")),
        check_vma=False,
    )
```

```python
import functools

import jax
import jax.numpy as jnp
from jax import lax
from jax.experimental import pallas as pl
from jax.experimental.pallas import tpu as pltpu
from jax.sharding import PartitionSpec as P

F32 = jnp.float32
BF16 = jnp.bfloat16
ROWS = 8


def split(x):
    hi = x.astype(BF16)
    return hi, (x - hi.astype(F32)).astype(BF16)


def stacked(x):
    hi = x.astype(BF16).astype(F32)
    return jnp.concatenate([hi, x - hi], axis=0).astype(BF16)


def dot2(x, pieces, dims):
    both = stacked(x)
    total = sum(
        lax.dot_general(both, piece, (dims, ((), ())), preferred_element_type=F32)
        for piece in pieces
    )
    return total[: x.shape[0]] + total[x.shape[0] :]


ALONG = ((1,), (1,))
ACROSS = ((1,), (0,))


def kernel(
    tiles,
    spans,
    symbols,
    emission_hbm,
    decay_hbm,
    left_hbm,
    right_hbm,
    initial_hbm,
    packed,
    emission,
    decay,
    left,
    right,
    entry,
    closing,
    side,
    kbuf,
    rbuf,
    gown,
    gbuf,
    kfull,
    pbuf,
    pall,
    load_sem,
    rs_send,
    rs_recv,
    ag_send,
    ag_recv,
    p_send,
    p_recv,
    pass_send,
    pass_recv,
):
    me = lax.axis_index("tm")
    span = lax.axis_index("state")
    frames = symbols.shape[0]
    rank, cells = right.shape
    width = kfull.shape[1]
    share = rank // tiles
    states = cells * tiles
    pairs = [(t, s) for s in range(frames) for t in range(s + 1, frames)]
    sums = [(t, s) for s in range(frames) for t in range(s + 1, frames + 1)]

    barrier = pltpu.get_barrier_semaphore()
    peers = [lax.rem(me + k, tiles) for k in range(tiles)]
    for k in range(1, tiles):
        pl.semaphore_signal(barrier, inc=1, device_id={"tm": peers[k]})
    turns = sorted({1 % spans, (spans - 1) % spans} - {0})
    for k in turns:
        pl.semaphore_signal(barrier, inc=1, device_id={"state": lax.rem(span + k, spans)})

    loads = [
        pltpu.make_async_copy(src, dst, load_sem.at[i])
        for i, (src, dst) in enumerate(
            (
                (emission_hbm, emission),
                (decay_hbm, decay),
                (left_hbm.at[0], left),
                (right_hbm.at[0], right),
            )
        )
    ]
    for load in loads:
        load.start()

    @pl.when(span == 0)
    def _():
        copy = pltpu.make_async_copy(initial_hbm, entry, load_sem.at[4])
        copy.start()
        copy.wait()

    row_id = lax.broadcasted_iota(jnp.int32, (ROWS, emission.shape[1]), 0)
    column_id = lax.broadcasted_iota(jnp.int32, (ROWS, emission.shape[1]), 1)
    wanted = jnp.full(row_id.shape, -1, jnp.int32)
    for t in range(frames):
        wanted = jnp.where(row_id == t, symbols[t], wanted)
    onehot = jnp.where(wanted == column_id, 1.0, 0.0).astype(BF16)
    for load in loads:
        load.wait()
    emitted = sum(
        lax.dot_general(onehot, piece, (ALONG, ((), ())), preferred_element_type=F32)
        for piece in split(emission[...])
    )
    emit = [emitted[t : t + 1] for t in range(frames)]
    grow = [emit[t] * decay[...] for t in range(frames)]
    scaled = left[...] * (1.0 / states)
    scaled_pieces = split(scaled)

    def send_projection():
        row = entry[...]
        rows = [row]
        for t in range(frames):
            row = row * grow[t]
            rows.append(row)
        rows += [jnp.zeros_like(row)] * (ROWS - len(rows))
        reached = jnp.concatenate(rows, axis=0)
        pbuf[:, :rank] = dot2(reached, scaled_pieces, ALONG)
        pbuf[:, rank:] = jnp.broadcast_to(
            jnp.sum(reached, axis=1, keepdims=True), (ROWS, pbuf.shape[1] - rank)
        )
        for k in range(1, tiles):
            p_copy(k).start()

    def p_copy(k):
        return pltpu.make_async_remote_copy(
            pbuf, pall.at[k - 1], p_send.at[k - 1], p_recv.at[k - 1], device_id={"tm": peers[k]}
        )

    def rs_copy(k):
        return pltpu.make_async_remote_copy(
            kbuf.at[peers[k]],
            rbuf.at[k - 1],
            rs_send.at[k - 1],
            rs_recv.at[k - 1],
            device_id={"tm": peers[k]},
        )

    def ag_copy(k):
        return pltpu.make_async_remote_copy(
            gown, gbuf.at[me], ag_send.at[k - 1], ag_recv.at[k - 1], device_id={"tm": peers[k]}
        )

    def pass_copy():
        return pltpu.make_async_remote_copy(
            closing, entry, pass_send, pass_recv, device_id={"state": lax.rem(span + 1, spans)}
        )

    reach = {}
    for s in range(frames):
        weight = emit[s]
        reach[s + 1, s] = weight
        for t in range(s + 1, frames):
            weight = weight * grow[t]
            reach[t + 1, s] = weight
    for i, pair in enumerate(pairs):
        side[i * rank : (i + 1) * rank] = reach[pair] * scaled
    base = len(pairs) * rank
    side[base:] = jnp.zeros((width - base, cells), F32)
    for i, pair in enumerate(sums):
        side[base + i : base + i + 1] = reach[pair]

    coupling = dot2(right[...], split(side[...]), ALONG)
    for j in range(tiles):
        kbuf[j] = coupling[j * share : (j + 1) * share]

    pl.semaphore_wait(barrier, tiles - 1 + len(turns))

    @pl.when(span == 0)
    def _():
        send_projection()

    for k in range(1, tiles):
        rs_copy(k).start()
    total = kbuf[me]
    for k in range(1, tiles):
        rs_copy(k).wait_recv()
        total = total + rbuf[k - 1]
    gown[...] = total
    for k in range(1, tiles):
        ag_copy(k).start()
    gbuf[me] = total
    for k in range(1, tiles):
        ag_copy(k).wait_recv()
    for j in range(tiles):
        kfull[j * share : (j + 1) * share] = gbuf[j]
    matrices = {
        pair: split(kfull[:, i * rank : (i + 1) * rank]) for i, pair in enumerate(pairs)
    }
    sum_matrix = split(kfull[:, base:])

    @pl.when(span > 0)
    def _():
        pass_copy().wait_recv()
        send_projection()

    projected = pbuf[...]
    for k in range(1, tiles):
        p_copy(k).wait_recv()
        projected = projected + pall[k - 1]
    mix = projected[:, :rank]
    mix_row = lax.broadcasted_iota(jnp.int32, mix.shape, 0)
    mix = jnp.where(mix_row < frames, mix, 0.0)
    for s in range(frames - 1):
        for t in range(s + 1, frames):
            term = dot2(mix, matrices[t, s], ACROSS)[s : s + 1]
            mix = mix + jnp.where(mix_row == t, term, 0.0)
    lifted = dot2(mix, split(right[...]), ACROSS)
    belief = entry[...]
    kept = []
    for t in range(frames):
        belief = grow[t] * belief + emit[t] * lifted[t : t + 1]
        kept.append(belief)
    if spans > 1:
        closing[...] = belief

        @pl.when(span < spans - 1)
        def _():
            pass_copy().start()

    parts = dot2(mix, sum_matrix, ACROSS)
    part_row = lax.broadcasted_iota(jnp.int32, parts.shape, 0)
    part_column = lax.broadcasted_iota(jnp.int32, parts.shape, 1)
    mass = [projected[0:1, rank : rank + 1]]
    for t in range(1, frames + 1):
        hit = jnp.zeros(parts.shape, jnp.bool_)
        for i, (u, s) in enumerate(sums):
            if u == t:
                hit = hit | ((part_row == s) & (part_column == i))
        mass.append(
            projected[t : t + 1, rank : rank + 1]
            + jnp.sum(jnp.where(hit, parts, 0.0), keepdims=True)
        )
    lane = lax.broadcasted_iota(jnp.int32, (1, 128), 1)
    levels = jnp.ones(lane.shape, F32)
    for t in range(frames):
        packed[t : t + 1] = kept[t] * (states / mass[t + 1])
        levels = jnp.where(lane == t, mass[t + 1] / mass[t], levels)
    packed[frames : frames + 1, :128] = jnp.log(levels)

    for k in range(1, tiles):
        p_copy(k).wait_send()
        rs_copy(k).wait_send()
        ag_copy(k).wait_send()
    if spans > 1:

        @pl.when(span < spans - 1)
        def _():
            pass_copy().wait_send()


def unpack(packed, beliefs_out, logs_out):
    frames = beliefs_out.shape[0]
    beliefs_out[...] = packed[:frames]
    logs_out[...] = packed[frames, :frames]


def solution(mesh):
    tiles, spans = mesh.shape["tm"], mesh.shape["state"]

    def per_device(symbols, emission, decay, left_factor, right_factor, initial):
        frames = symbols.shape[0]
        rank, cells = left_factor.shape[1:]
        pair_count = frames * (frames - 1) // 2
        sum_count = frames * (frames + 1) // 2
        width = -(-(pair_count * rank + sum_count) // 128) * 128
        share = rank // tiles
        vmem, dma = pltpu.VMEM, pltpu.SemaphoreType.DMA
        others = tiles - 1
        packed = pl.pallas_call(
            functools.partial(kernel, tiles, spans),
            out_shape=vmem((ROWS, cells), F32),
            in_specs=[pl.BlockSpec(memory_space=pltpu.SMEM)]
            + [pl.BlockSpec(memory_space=pltpu.HBM)] * 5,
            out_specs=pl.BlockSpec(memory_space=vmem),
            scratch_shapes=[
                vmem(emission.shape, F32),
                vmem(decay.shape, F32),
                vmem((rank, cells), F32),
                vmem((rank, cells), F32),
                vmem((1, cells), F32),
                vmem((1, cells), F32),
                vmem((width, cells), F32),
                vmem((tiles, share, width), F32),
                vmem((others, share, width), F32),
                vmem((share, width), F32),
                vmem((tiles, share, width), F32),
                vmem((rank, width), F32),
                vmem((ROWS, 128), F32),
                vmem((others, ROWS, 128), F32),
                dma((5,)),
                dma((others,)),
                dma((others,)),
                dma((others,)),
                dma((others,)),
                dma((others,)),
                dma((others,)),
                dma(()),
                dma(()),
            ],
            compiler_params=pltpu.CompilerParams(collective_id=0, has_side_effects=True),
        )(symbols, emission, decay, left_factor, right_factor, initial.reshape(1, cells))
        return pl.pallas_call(
            unpack,
            out_shape=(
                jax.ShapeDtypeStruct((frames, cells), F32),
                jax.ShapeDtypeStruct((frames,), F32),
            ),
            in_specs=[pl.BlockSpec(memory_space=vmem)],
            out_specs=(pl.BlockSpec(memory_space=vmem),) * 2,
            compiler_params=pltpu.CompilerParams(vmem_limit_bytes=16 * 2**20),
        )(packed)

    return jax.shard_map(
        per_device,
        mesh=mesh,
        in_specs=(
            P("state"),
            P("tm", None),
            P("state", "tm"),
            P("state", None, "tm"),
            P("state", None, "tm"),
            P("tm"),
        ),
        out_specs=(P("state", "tm"), P("state")),
        check_vma=False,
    )
```

```python
import functools

import jax
import jax.numpy as jnp
from jax import lax
from jax.experimental import pallas as pl
from jax.experimental.pallas import tpu as pltpu
from jax.sharding import PartitionSpec as P

F32 = jnp.float32
BF16 = jnp.bfloat16
ROWS = 8


def split(x):
    hi = x.astype(BF16)
    return hi, (x - hi.astype(F32)).astype(BF16)


def stacked(x):
    hi = x.astype(BF16).astype(F32)
    return jnp.concatenate([hi, x - hi], axis=0).astype(BF16)


def dot2(x, pieces, dims):
    both = stacked(x)
    total = sum(
        lax.dot_general(both, piece, (dims, ((), ())), preferred_element_type=F32)
        for piece in pieces
    )
    return total[: x.shape[0]] + total[x.shape[0] :]


ALONG = ((1,), (1,))
ACROSS = ((1,), (0,))
LAST = 1


def kernel(
    tiles,
    symbols,
    emission_hbm,
    decay_hbm,
    left_hbm,
    right_hbm,
    initial_hbm,
    packed,
    emission,
    decay,
    left,
    right,
    entry,
    side,
    first_pieces,
    first_parts,
    first_own,
    first_all,
    first_full,
    last_pieces,
    last_parts,
    last_own,
    last_all,
    last_full,
    pbuf,
    first_proj,
    last_proj,
    pace,
    first_pace,
    first_right,
    hand,
    handed,
    mass_out,
    mass_in,
    load_sem,
    fs_send,
    fs_recv,
    fg_send,
    fg_recv,
    ls_send,
    ls_recv,
    lg_send,
    lg_recv,
    fp_send,
    fp_recv,
    lp_send,
    lp_recv,
    chip_send,
    chip_recv,
    clear,
):
    me = lax.axis_index("tm")
    span = lax.axis_index("state")
    frames = symbols.shape[0]
    rank, cells = right.shape
    share = rank // tiles
    states = cells * tiles
    pairs = [(t, s) for s in range(frames) for t in range(s + 1, frames)]
    sums = [(t, s) for s in range(frames) for t in range(s + 1, frames + 1)]
    base = len(pairs) * rank
    width = last_full.shape[1]
    peers = [lax.rem(me + k, tiles) for k in range(tiles)]
    half = rank + 32

    barrier = pltpu.get_barrier_semaphore()

    @pl.when(span < LAST)
    def _():
        for k in range(tiles):
            pl.semaphore_signal(barrier, inc=1, device_id={"tm": peers[k], "state": LAST})

    @pl.when(span == LAST)
    def _():
        for k in range(1, tiles):
            pl.semaphore_signal(barrier, inc=1, device_id={"tm": peers[k], "state": LAST})
        for k in range(tiles):
            pl.semaphore_signal(barrier, inc=1, device_id={"tm": peers[k], "state": 0})

    loads = [
        pltpu.make_async_copy(src, dst, load_sem.at[i])
        for i, (src, dst) in enumerate(
            (
                (emission_hbm, emission),
                (decay_hbm, decay),
                (left_hbm.at[0], left),
                (right_hbm.at[0], right),
                (initial_hbm, entry),
            )
        )
    ]
    for load in loads:
        load.start()

    def remote(src, dst, send, recv, tile, state):
        return pltpu.make_async_remote_copy(
            src, dst, send, recv, device_id={"tm": tile, "state": state}
        )

    def first_scatter(k):
        return remote(
            first_pieces.at[peers[k]], first_parts.at[k], fs_send.at[k], fs_recv.at[k], peers[k], LAST
        )

    def first_project(k):
        return remote(pbuf, first_proj.at[k], fp_send.at[k], fp_recv.at[k], peers[k], LAST)

    def first_gather(k):
        return remote(
            first_own, first_all.at[me], fg_send.at[k - 1], fg_recv.at[k - 1], peers[k], LAST
        )

    def last_scatter(k):
        return remote(
            last_pieces.at[peers[k]],
            last_parts.at[k - 1],
            ls_send.at[k - 1],
            ls_recv.at[k - 1],
            peers[k],
            LAST,
        )

    def last_gather(k):
        return remote(
            last_own, last_all.at[me], lg_send.at[k - 1], lg_recv.at[k - 1], peers[k], LAST
        )

    def last_project(k):
        return remote(
            pbuf, last_proj.at[k - 1], lp_send.at[k - 1], lp_recv.at[k - 1], peers[k], LAST
        )

    def give(i):
        src, dst, state = (
            (right, first_right, LAST),
            (pace, first_pace, LAST),
            (hand, handed, 0),
            (mass_out, mass_in, 0),
        )[i]
        return remote(src, dst, chip_send.at[i], chip_recv.at[i], me, state)

    row_id = lax.broadcasted_iota(jnp.int32, (ROWS, emission.shape[1]), 0)
    column_id = lax.broadcasted_iota(jnp.int32, (ROWS, emission.shape[1]), 1)
    wanted = jnp.full(row_id.shape, -1, jnp.int32)
    for t in range(frames):
        wanted = jnp.where(row_id == t, symbols[t], wanted)
    onehot = jnp.where(wanted == column_id, 1.0, 0.0).astype(BF16)
    for load in loads:
        load.wait()
    emitted = sum(
        lax.dot_general(onehot, piece, (ALONG, ((), ())), preferred_element_type=F32)
        for piece in split(emission[...])
    )
    emit = [emitted[t : t + 1] for t in range(frames)]
    grow = [emit[t] * decay[...] for t in range(frames)]
    scaled = left[...] * (1.0 / states)
    scaled_pieces = split(scaled)
    for t in range(frames):
        pace[t : t + 1] = emit[t]
        pace[frames + t : frames + t + 1] = grow[t]

    def projections(row):
        rows = [row]
        for t in range(frames):
            row = row * grow[t]
            rows.append(row)
        rows += [jnp.zeros_like(row)] * (ROWS - len(rows))
        reached = jnp.concatenate(rows, axis=0)
        pbuf[:, :rank] = dot2(reached, scaled_pieces, ALONG)
        pbuf[:, rank:half] = jnp.broadcast_to(
            jnp.sum(reached, axis=1, keepdims=True), (ROWS, half - rank)
        )

    def couplings():
        reach = {}
        for s in range(frames):
            weight = emit[s]
            reach[s + 1, s] = weight
            for t in range(s + 1, frames):
                weight = weight * grow[t]
                reach[t + 1, s] = weight
        for i, pair in enumerate(pairs):
            side[i * rank : (i + 1) * rank] = reach[pair] * scaled
        side[base:] = jnp.zeros((width - base, cells), F32)
        for i, pair in enumerate(sums):
            side[base + i : base + i + 1] = reach[pair]
        return dot2(right[...], split(side[...]), ALONG)

    def solve(mix, full):
        mix_row = lax.broadcasted_iota(jnp.int32, mix.shape, 0)
        mix = jnp.where(mix_row < frames, mix, 0.0)
        for s in range(frames - 1):
            for i, (t, u) in enumerate(pairs):
                if u == s:
                    matrix = split(full[:, i * rank : (i + 1) * rank])
                    term = dot2(mix, matrix, ACROSS)[s : s + 1]
                    mix = mix + jnp.where(mix_row == t, term, 0.0)
        return mix

    def advance(belief, emits, grows, lifted):
        kept = []
        for t in range(frames):
            belief = grows[t] * belief + emits[t] * lifted[t : t + 1]
            kept.append(belief)
        return kept

    def write(kept, mass):
        lane = lax.broadcasted_iota(jnp.int32, (1, 128), 1)
        levels = jnp.ones(lane.shape, F32)
        for t in range(frames):
            packed[t : t + 1] = kept[t] * (states / mass[t + 1])
            levels = jnp.where(lane == t, mass[t + 1] / mass[t], levels)
        packed[frames : frames + 1, :128] = jnp.log(levels)

    coupling = couplings()

    @pl.when(span < LAST)
    def _():
        for j in range(tiles):
            first_pieces[j] = coupling[j * share : (j + 1) * share, :base]
        projections(entry[...])
        pbuf[:, half:] = jnp.zeros((ROWS, pbuf.shape[1] - half), F32)
        pl.semaphore_wait(barrier, tiles)
        for k in range(tiles):
            first_scatter(k).start()
        for k in range(tiles):
            first_project(k).start()
        give(0).start()
        give(1).start()
        for k in range(tiles):
            first_scatter(k).wait_send()
        pl.semaphore_signal(clear, inc=1, device_id={"tm": me, "state": LAST})
        for k in range(tiles):
            first_project(k).wait_send()
        give(0).wait_send()
        give(1).wait_send()
        give(2).wait_recv()
        kept = [handed[t : t + 1] for t in range(frames)]
        mass = [handed[frames : frames + 1, :1]]
        give(3).wait_recv()
        mass += [mass_in[t : t + 1, half : half + 1] for t in range(frames - 1)]
        mass += [mass_in[0:1, rank : rank + 1]]
        write(kept, mass)

    @pl.when(span == LAST)
    def _():
        for j in range(tiles):
            last_pieces[j] = coupling[j * share : (j + 1) * share]
        pl.semaphore_wait(barrier, 2 * tiles - 1)
        pl.semaphore_wait(clear, 1)
        for k in range(1, tiles):
            last_scatter(k).start()
        total = jnp.zeros(first_own.shape, F32)
        for k in range(tiles):
            first_scatter(k).wait_recv()
            total = total + first_parts[k]
        first_own[...] = total
        for k in range(1, tiles):
            first_gather(k).start()
        first_all[me] = total
        total = last_pieces[me]
        for k in range(1, tiles):
            last_scatter(k).wait_recv()
            total = total + last_parts[k - 1]
        last_own[...] = total
        for k in range(1, tiles):
            last_gather(k).start()
        last_all[me] = total

        projected = jnp.zeros(pbuf.shape, F32)
        for k in range(tiles):
            first_project(k).wait_recv()
            projected = projected + first_proj[k]
        give(0).wait_recv()
        give(1).wait_recv()
        for k in range(1, tiles):
            first_gather(k).wait_recv()
        for j in range(tiles):
            first_full[j * share : (j + 1) * share] = first_all[j]
        mix = solve(projected[:, :rank], first_full)
        lifted = dot2(mix, split(first_right[...]), ACROSS)
        emits = [first_pace[t : t + 1] for t in range(frames)]
        grows = [first_pace[frames + t : frames + t + 1] for t in range(frames)]
        kept = advance(entry[...], emits, grows, lifted)
        belief = kept[-1]
        projections(belief)
        partial = jnp.concatenate(
            kept[:-1] + [jnp.zeros((ROWS + 1 - frames, cells), F32)], axis=0
        )
        pbuf[:, half:] = jnp.broadcast_to(
            jnp.sum(partial, axis=1, keepdims=True), (ROWS, pbuf.shape[1] - half)
        )
        for k in range(1, tiles):
            last_project(k).start()
        for t in range(frames):
            hand[t : t + 1] = kept[t]
        hand[frames : frames + 1] = jnp.broadcast_to(projected[0:1, rank : rank + 1], (1, cells))
        give(2).start()

        for k in range(1, tiles):
            last_gather(k).wait_recv()
        for j in range(tiles):
            last_full[j * share : (j + 1) * share] = last_all[j]
        projected = pbuf[...]
        for k in range(1, tiles):
            last_project(k).wait_recv()
            projected = projected + last_proj[k - 1]
        mass_out[...] = projected
        give(3).start()
        mix = solve(projected[:, :rank], last_full)
        lifted = dot2(mix, split(right[...]), ACROSS)
        kept = advance(belief, emit, grow, lifted)
        parts = dot2(mix, split(last_full[:, base:]), ACROSS)
        part_row = lax.broadcasted_iota(jnp.int32, parts.shape, 0)
        part_column = lax.broadcasted_iota(jnp.int32, parts.shape, 1)
        mass = [projected[0:1, rank : rank + 1]]
        for t in range(1, frames + 1):
            hit = jnp.zeros(parts.shape, jnp.bool_)
            for i, (u, s) in enumerate(sums):
                if u == t:
                    hit = hit | ((part_row == s) & (part_column == i))
            mass.append(
                projected[t : t + 1, rank : rank + 1]
                + jnp.sum(jnp.where(hit, parts, 0.0), keepdims=True)
            )
        write(kept, mass)
        for k in range(1, tiles):
            last_scatter(k).wait_send()
            first_gather(k).wait_send()
            last_gather(k).wait_send()
            last_project(k).wait_send()
        give(2).wait_send()
        give(3).wait_send()


def unpack(packed, beliefs_out, logs_out):
    frames = beliefs_out.shape[0]
    beliefs_out[...] = packed[:frames]
    logs_out[...] = packed[frames, :frames]


def solution(mesh):
    tiles = mesh.shape["tm"]
    assert mesh.shape["state"] == LAST + 1

    def per_device(symbols, emission, decay, left_factor, right_factor, initial):
        frames = symbols.shape[0]
        rank, cells = left_factor.shape[1:]
        pair_count = frames * (frames - 1) // 2
        sum_count = frames * (frames + 1) // 2
        base = pair_count * rank
        width = -(-(pair_count * rank + sum_count) // 128) * 128
        share = rank // tiles
        vmem, dma = pltpu.VMEM, pltpu.SemaphoreType.DMA
        others = tiles - 1
        packed = pl.pallas_call(
            functools.partial(kernel, tiles),
            out_shape=vmem((ROWS, cells), F32),
            in_specs=[pl.BlockSpec(memory_space=pltpu.SMEM)]
            + [pl.BlockSpec(memory_space=pltpu.HBM)] * 5,
            out_specs=pl.BlockSpec(memory_space=vmem),
            scratch_shapes=[
                vmem(emission.shape, F32),
                vmem(decay.shape, F32),
                vmem((rank, cells), F32),
                vmem((rank, cells), F32),
                vmem((1, cells), F32),
                vmem((width, cells), F32),
                vmem((tiles, share, base), F32),
                vmem((tiles, share, base), F32),
                vmem((share, base), F32),
                vmem((tiles, share, base), F32),
                vmem((rank, base), F32),
                vmem((tiles, share, width), F32),
                vmem((others, share, width), F32),
                vmem((share, width), F32),
                vmem((tiles, share, width), F32),
                vmem((rank, width), F32),
                vmem((ROWS, 128), F32),
                vmem((tiles, ROWS, 128), F32),
                vmem((others, ROWS, 128), F32),
                vmem((2 * frames, cells), F32),
                vmem((2 * frames, cells), F32),
                vmem((rank, cells), F32),
                vmem((ROWS, cells), F32),
                vmem((ROWS, cells), F32),
                vmem((ROWS, 128), F32),
                vmem((ROWS, 128), F32),
                dma((5,)),
                dma((tiles,)),
                dma((tiles,)),
                dma((others,)),
                dma((others,)),
                dma((others,)),
                dma((others,)),
                dma((others,)),
                dma((others,)),
                dma((tiles,)),
                dma((tiles,)),
                dma((others,)),
                dma((others,)),
                dma((4,)),
                dma((4,)),
                pltpu.SemaphoreType.REGULAR,
            ],
            compiler_params=pltpu.CompilerParams(collective_id=0, has_side_effects=True),
        )(symbols, emission, decay, left_factor, right_factor, initial.reshape(1, cells))
        return pl.pallas_call(
            unpack,
            out_shape=(
                jax.ShapeDtypeStruct((frames, cells), F32),
                jax.ShapeDtypeStruct((frames,), F32),
            ),
            in_specs=[pl.BlockSpec(memory_space=vmem)],
            out_specs=(pl.BlockSpec(memory_space=vmem),) * 2,
            compiler_params=pltpu.CompilerParams(vmem_limit_bytes=16 * 2**20),
        )(packed)

    return jax.shard_map(
        per_device,
        mesh=mesh,
        in_specs=(
            P("state"),
            P("tm", None),
            P("state", "tm"),
            P("state", None, "tm"),
            P("state", None, "tm"),
            P("tm"),
        ),
        out_specs=(P("state", "tm"), P("state")),
        check_vma=False,
    )
```

```python
import functools

import jax
import jax.numpy as jnp
from jax import lax
from jax.experimental import pallas as pl
from jax.experimental.pallas import tpu as pltpu
from jax.sharding import PartitionSpec as P

F32 = jnp.float32
BF16 = jnp.bfloat16
ROWS = 8


def split(x):
    hi = x.astype(BF16)
    return hi, (x - hi.astype(F32)).astype(BF16)


def stacked(x):
    hi = x.astype(BF16).astype(F32)
    return jnp.concatenate([hi, x - hi], axis=0).astype(BF16)


def dot2(x, pieces, dims):
    both = stacked(x)
    total = sum(
        lax.dot_general(both, piece, (dims, ((), ())), preferred_element_type=F32)
        for piece in pieces
    )
    return total[: x.shape[0]] + total[x.shape[0] :]


ALONG = ((1,), (1,))
ACROSS = ((1,), (0,))
LAST = 1


def kernel(
    tiles,
    symbols,
    emission_hbm,
    decay_hbm,
    left_hbm,
    right_hbm,
    initial_hbm,
    packed,
    emission,
    decay,
    left,
    right,
    entry,
    side,
    first_pieces,
    first_parts,
    first_own,
    first_all,
    first_full,
    last_pieces,
    last_parts,
    last_own,
    last_all,
    last_full,
    first_row,
    first_proj,
    mid_rows,
    mid_proj,
    pbuf,
    last_proj,
    pace,
    first_pace,
    first_right,
    first_left,
    lift_pieces,
    probe_pieces,
    hand,
    handed,
    mass_out,
    mass_in,
    load_sem,
    fs_send,
    fs_recv,
    fg_send,
    fg_recv,
    ls_send,
    ls_recv,
    lg_send,
    lg_recv,
    fp_send,
    fp_recv,
    mp_send,
    mp_recv,
    lp_send,
    lp_recv,
    chip_send,
    chip_recv,
    clear,
):
    me = lax.axis_index("tm")
    span = lax.axis_index("state")
    frames = symbols.shape[0]
    rank, cells = right.shape
    share = rank // tiles
    states = cells * tiles
    pairs = [(t, s) for s in range(frames) for t in range(s + 1, frames)]
    sums = [(t, s) for s in range(frames) for t in range(s + 1, frames + 1)]
    base = len(pairs) * rank
    width = last_full.shape[1]
    first_width = first_full.shape[1]
    skip = (frames - 1) * rank // 128 * 128
    peers = [lax.rem(me + k, tiles) for k in range(tiles)]
    half = rank + 32

    loads = [
        pltpu.make_async_copy(src, dst, load_sem.at[i])
        for i, (src, dst) in enumerate(
            (
                (emission_hbm, emission),
                (decay_hbm, decay),
                (left_hbm.at[0], left),
                (right_hbm.at[0], right),
                (initial_hbm, entry),
            )
        )
    ]
    for load in loads:
        load.start()

    barrier = pltpu.get_barrier_semaphore()

    @pl.when(span < LAST)
    def _():
        for k in range(tiles):
            pl.semaphore_signal(barrier, inc=1, device_id={"tm": peers[k], "state": LAST})

    @pl.when(span == LAST)
    def _():
        for k in range(1, tiles):
            pl.semaphore_signal(barrier, inc=1, device_id={"tm": peers[k], "state": LAST})
        for k in range(tiles):
            pl.semaphore_signal(barrier, inc=1, device_id={"tm": peers[k], "state": 0})

    def remote(src, dst, send, recv, tile, state):
        return pltpu.make_async_remote_copy(
            src, dst, send, recv, device_id={"tm": tile, "state": state}
        )

    def first_scatter(k):
        return remote(
            first_pieces.at[peers[k]], first_parts.at[k], fs_send, fs_recv, peers[k], LAST
        )

    def first_project(k):
        return remote(first_row, first_proj.at[k], fp_send, fp_recv, peers[k], LAST)

    def first_gather(k):
        return remote(first_own, first_all.at[me], fg_send, fg_recv, peers[k], LAST)

    def mid_project(k):
        return remote(mid_rows, mid_proj.at[k - 1], mp_send, mp_recv, peers[k], LAST)

    def last_scatter(k):
        return remote(
            last_pieces.at[peers[k]], last_parts.at[k - 1], ls_send, ls_recv, peers[k], LAST
        )

    def last_gather(k):
        return remote(last_own, last_all.at[me], lg_send, lg_recv, peers[k], LAST)

    def last_project(k):
        return remote(pbuf, last_proj.at[k - 1], lp_send, lp_recv, peers[k], LAST)

    def landed(ref, sem):
        pltpu.make_async_copy(ref, ref, sem).wait()

    def give(i):
        src, dst, state = (
            (right, first_right, LAST),
            (pace, first_pace, LAST),
            (hand, handed, 0),
            (mass_out, mass_in, 0),
            (left, first_left, LAST),
        )[i]
        return remote(src, dst, chip_send.at[i], chip_recv.at[i], me, state)

    others = pl.ds(0, tiles - 1)

    row_id = lax.broadcasted_iota(jnp.int32, (ROWS, emission.shape[1]), 0)
    column_id = lax.broadcasted_iota(jnp.int32, (ROWS, emission.shape[1]), 1)
    wanted = jnp.full(row_id.shape, -1, jnp.int32)
    for t in range(frames):
        wanted = jnp.where(row_id == t, symbols[t], wanted)
    onehot = jnp.where(wanted == column_id, 1.0, 0.0).astype(BF16)
    for load in loads:
        load.wait()
    emitted = sum(
        lax.dot_general(onehot, piece, (ALONG, ((), ())), preferred_element_type=F32)
        for piece in split(emission[...])
    )
    emit = [emitted[t : t + 1] for t in range(frames)]
    grow = [emit[t] * decay[...] for t in range(frames)]
    scaled = left[...] * (1.0 / states)
    scaled_pieces = split(scaled)
    for t in range(frames):
        pace[t : t + 1] = emit[t]
        pace[frames + t : frames + t + 1] = grow[t]

    def filled(rows):
        return jnp.concatenate(rows + [jnp.zeros_like(rows[0])] * (ROWS - len(rows)), axis=0)

    def projections(row):
        rows = [row]
        for t in range(frames):
            row = row * grow[t]
            rows.append(row)
        reached = filled(rows)
        pbuf[:, :rank] = dot2(reached, scaled_pieces, ALONG)
        pbuf[:, rank:half] = jnp.broadcast_to(
            jnp.sum(reached, axis=1, keepdims=True), (ROWS, half - rank)
        )

    def couplings():
        reach = {}
        for s in range(frames):
            weight = emit[s]
            reach[s + 1, s] = weight
            for t in range(s + 1, frames):
                weight = weight * grow[t]
                reach[t + 1, s] = weight
        for i, pair in enumerate(pairs):
            side[i * rank : (i + 1) * rank] = reach[pair] * scaled
        side[base:] = jnp.zeros((width - base, cells), F32)
        for i, pair in enumerate(sums):
            side[base + i : base + i + 1] = reach[pair]
        return dot2(right[...], split(side[...]), ALONG)

    def solve(mix, full, origin=0, start=0):
        mix_row = lax.broadcasted_iota(jnp.int32, mix.shape, 0)
        mix = jnp.where(mix_row < frames, mix, 0.0)
        for s in range(start, frames - 1):
            for i, (t, u) in enumerate(pairs):
                if u == s:
                    matrix = split(full[:, i * rank - origin : (i + 1) * rank - origin])
                    term = dot2(mix, matrix, ACROSS)[s : s + 1]
                    mix = mix + jnp.where(mix_row == t, term, 0.0)
        return mix

    def advance(belief, emits, grows, lifted):
        kept = []
        for t in range(frames):
            belief = grows[t] * belief + emits[t] * lifted[t : t + 1]
            kept.append(belief)
        return kept

    def write(kept, mass):
        lane = lax.broadcasted_iota(jnp.int32, (1, 128), 1)
        levels = jnp.ones(lane.shape, F32)
        for t in range(frames):
            packed[t : t + 1] = kept[t] * (states / mass[t + 1])
            levels = jnp.where(lane == t, mass[t + 1] / mass[t], levels)
        packed[frames : frames + 1, :128] = jnp.log(levels)

    coupling = couplings()

    @pl.when(span < LAST)
    def _():
        for j in range(tiles):
            first_pieces[j] = coupling[j * share : (j + 1) * share, skip : skip + first_width]
        row = entry[...]
        first_row[:, :rank] = dot2(filled([row]), scaled_pieces, ALONG)[:1]
        first_row[:, rank:] = jnp.broadcast_to(
            jnp.sum(row, axis=1, keepdims=True), (1, first_row.shape[1] - rank)
        )
        pl.semaphore_wait(barrier, tiles)
        for k in reversed(range(tiles)):
            first_project(k).start()
        for k in reversed(range(tiles)):
            first_scatter(k).start()
        for i in (0, 1, 4):
            give(i).start()
        landed(first_pieces, fs_send)
        pl.semaphore_signal(clear, inc=1, device_id={"tm": me, "state": LAST})
        landed(first_proj, fp_send)
        for i in (0, 1, 4):
            give(i).wait_send()
        give(2).wait_recv()
        kept = [handed[t : t + 1] for t in range(frames)]
        mass = [handed[frames : frames + 1, :1]]
        give(3).wait_recv()
        mass += [mass_in[t : t + 1, half : half + 1] for t in range(frames - 1)]
        mass += [mass_in[0:1, rank : rank + 1]]
        write(kept, mass)

    @pl.when(span == LAST)
    def _():
        for j in range(tiles):
            last_pieces[j] = coupling[j * share : (j + 1) * share]
        pl.semaphore_wait(barrier, 2 * tiles - 1)
        pl.semaphore_wait(clear, 1)
        for k in range(1, tiles):
            last_scatter(k).start()
        for i in (0, 1, 4):
            give(i).wait_recv()
        for i, piece in enumerate(split(first_right[...])):
            lift_pieces[i] = piece
        for i, piece in enumerate(split(first_left[...] * (1.0 / states))):
            probe_pieces[i] = piece
        emits = [first_pace[t : t + 1] for t in range(frames)]
        grows = [first_pace[frames + t : frames + t + 1] for t in range(frames)]
        landed(first_proj, fp_recv)
        opening = first_proj[0]
        for k in range(1, tiles):
            opening = opening + first_proj[k]
        mix_first = jnp.broadcast_to(opening[:, :rank], (ROWS, rank))
        lifted = dot2(mix_first, (lift_pieces[0], lift_pieces[1]), ACROSS)
        second = grows[0] * entry[...] + emits[0] * lifted[:1]
        rows = [second]
        for t in range(1, frames - 1):
            rows.append(rows[-1] * grows[t])
        mid_rows[:, :rank] = dot2(filled(rows), (probe_pieces[0], probe_pieces[1]), ALONG)[
            :frames
        ]
        mid_rows[:, rank:] = jnp.zeros((frames, mid_rows.shape[1] - rank), F32)
        for k in range(1, tiles):
            mid_project(k).start()
        landed(first_parts, fs_recv)
        total = first_parts[0]
        for k in range(1, tiles):
            total = total + first_parts[k]
        first_own[...] = total
        for k in range(1, tiles):
            first_gather(k).start()
        first_all[me] = total
        landed(last_parts, ls_recv)
        total = last_pieces[me]
        for k in range(1, tiles):
            total = total + last_parts[k - 1]
        last_own[...] = total
        for k in range(1, tiles):
            last_gather(k).start()
        last_all[me] = total

        landed(mid_proj, mp_recv)
        later = mid_rows[...]
        for k in range(1, tiles):
            later = later + mid_proj[k - 1]
        mix = jnp.concatenate(
            [opening[:, :rank], later[: frames - 1, :rank]]
            + [jnp.zeros((1, rank), F32)] * (ROWS - frames),
            axis=0,
        )
        landed(first_all.at[others], fg_recv)
        for j in range(tiles):
            first_full[j * share : (j + 1) * share] = first_all[j]
        mix = solve(mix, first_full, skip, 1)
        lifted = dot2(mix, (lift_pieces[0], lift_pieces[1]), ACROSS)
        kept = [second]
        for t in range(1, frames):
            kept.append(grows[t] * kept[-1] + emits[t] * lifted[t : t + 1])
        belief = kept[-1]
        projections(belief)
        partial = jnp.concatenate(
            kept[:-1] + [jnp.zeros((ROWS + 1 - frames, cells), F32)], axis=0
        )
        pbuf[:, half:] = jnp.broadcast_to(
            jnp.sum(partial, axis=1, keepdims=True), (ROWS, pbuf.shape[1] - half)
        )
        for k in range(1, tiles):
            last_project(k).start()
        for t in range(frames):
            hand[t : t + 1] = kept[t]
        hand[frames : frames + 1] = jnp.broadcast_to(opening[:, rank : rank + 1], (1, cells))
        give(2).start()

        landed(last_all.at[others], lg_recv)
        for j in range(tiles):
            last_full[j * share : (j + 1) * share] = last_all[j]
        projected = pbuf[...]
        landed(last_proj, lp_recv)
        for k in range(1, tiles):
            projected = projected + last_proj[k - 1]
        mass_out[...] = projected
        give(3).start()
        mix = solve(projected[:, :rank], last_full)
        lifted = dot2(mix, split(right[...]), ACROSS)
        kept = advance(belief, emit, grow, lifted)
        parts = dot2(mix, split(last_full[:, base:]), ACROSS)
        part_row = lax.broadcasted_iota(jnp.int32, parts.shape, 0)
        part_column = lax.broadcasted_iota(jnp.int32, parts.shape, 1)
        mass = [projected[0:1, rank : rank + 1]]
        for t in range(1, frames + 1):
            hit = jnp.zeros(parts.shape, jnp.bool_)
            for i, (u, s) in enumerate(sums):
                if u == t:
                    hit = hit | ((part_row == s) & (part_column == i))
            mass.append(
                projected[t : t + 1, rank : rank + 1]
                + jnp.sum(jnp.where(hit, parts, 0.0), keepdims=True)
            )
        write(kept, mass)
        landed(last_parts, ls_send)
        landed(first_all.at[others], fg_send)
        landed(mid_proj, mp_send)
        landed(last_all.at[others], lg_send)
        landed(last_proj, lp_send)
        give(2).wait_send()
        give(3).wait_send()


def unpack(packed, beliefs_out, logs_out):
    frames = beliefs_out.shape[0]
    beliefs_out[...] = packed[:frames]
    logs_out[...] = packed[frames, :frames]


def solution(mesh):
    tiles = mesh.shape["tm"]
    assert mesh.shape["state"] == LAST + 1

    def per_device(symbols, emission, decay, left_factor, right_factor, initial):
        frames = symbols.shape[0]
        rank, cells = left_factor.shape[1:]
        pair_count = frames * (frames - 1) // 2
        sum_count = frames * (frames + 1) // 2
        base = pair_count * rank
        first_width = -(-base // 128) * 128 - (frames - 1) * rank // 128 * 128
        width = -(-(pair_count * rank + sum_count) // 128) * 128
        share = rank // tiles
        vmem, dma = pltpu.VMEM, pltpu.SemaphoreType.DMA
        others = tiles - 1
        packed = pl.pallas_call(
            functools.partial(kernel, tiles),
            out_shape=vmem((ROWS, cells), F32),
            in_specs=[pl.BlockSpec(memory_space=pltpu.SMEM)]
            + [pl.BlockSpec(memory_space=pltpu.HBM)] * 5,
            out_specs=pl.BlockSpec(memory_space=vmem),
            scratch_shapes=[
                vmem(emission.shape, F32),
                vmem(decay.shape, F32),
                vmem((rank, cells), F32),
                vmem((rank, cells), F32),
                vmem((1, cells), F32),
                vmem((width, cells), F32),
                vmem((tiles, share, first_width), F32),
                vmem((tiles, share, first_width), F32),
                vmem((share, first_width), F32),
                vmem((tiles, share, first_width), F32),
                vmem((rank, first_width), F32),
                vmem((tiles, share, width), F32),
                vmem((others, share, width), F32),
                vmem((share, width), F32),
                vmem((tiles, share, width), F32),
                vmem((rank, width), F32),
                vmem((1, 128), F32),
                vmem((tiles, 1, 128), F32),
                vmem((frames, 128), F32),
                vmem((others, frames, 128), F32),
                vmem((ROWS, 128), F32),
                vmem((others, ROWS, 128), F32),
                vmem((2 * frames, cells), F32),
                vmem((2 * frames, cells), F32),
                vmem((rank, cells), F32),
                vmem((rank, cells), F32),
                vmem((2, rank, cells), BF16),
                vmem((2, rank, cells), BF16),
                vmem((ROWS, cells), F32),
                vmem((ROWS, cells), F32),
                vmem((ROWS, 128), F32),
                vmem((ROWS, 128), F32),
                dma((5,)),
                *[dma(())] * 14,
                dma((5,)),
                dma((5,)),
                pltpu.SemaphoreType.REGULAR,
            ],
            compiler_params=pltpu.CompilerParams(collective_id=0, has_side_effects=True),
        )(symbols, emission, decay, left_factor, right_factor, initial.reshape(1, cells))
        return pl.pallas_call(
            unpack,
            out_shape=(
                jax.ShapeDtypeStruct((frames, cells), F32),
                jax.ShapeDtypeStruct((frames,), F32),
            ),
            in_specs=[pl.BlockSpec(memory_space=vmem)],
            out_specs=(pl.BlockSpec(memory_space=vmem),) * 2,
            compiler_params=pltpu.CompilerParams(vmem_limit_bytes=16 * 2**20),
        )(packed)

    return jax.shard_map(
        per_device,
        mesh=mesh,
        in_specs=(
            P("state"),
            P("tm", None),
            P("state", "tm"),
            P("state", None, "tm"),
            P("state", None, "tm"),
            P("tm"),
        ),
        out_specs=(P("state", "tm"), P("state")),
        check_vma=False,
    )
```

```python
import functools

import jax
import jax.numpy as jnp
from jax import lax
from jax.experimental import pallas as pl
from jax.experimental.pallas import tpu as pltpu
from jax.sharding import PartitionSpec as P

F32 = jnp.float32
BF16 = jnp.bfloat16
ROWS = 8


def split(x):
    hi = x.astype(BF16)
    return hi, (x - hi.astype(F32)).astype(BF16)


def stacked(x):
    hi = x.astype(BF16).astype(F32)
    return jnp.concatenate([hi, x - hi], axis=0).astype(BF16)


def dot2(x, pieces, dims):
    both = stacked(x)
    total = sum(
        lax.dot_general(both, piece, (dims, ((), ())), preferred_element_type=F32)
        for piece in pieces
    )
    return total[: x.shape[0]] + total[x.shape[0] :]


ALONG = ((1,), (1,))
ACROSS = ((1,), (0,))
LAST = 1


def kernel(
    tiles,
    symbols,
    emission_hbm,
    decay_hbm,
    left_hbm,
    right_hbm,
    initial_hbm,
    packed,
    emission,
    decay,
    left,
    right,
    entry,
    side,
    first_pieces,
    first_parts,
    first_own,
    first_all,
    first_full,
    last_pieces,
    last_parts,
    last_own,
    last_all,
    last_full,
    first_row,
    first_proj,
    mid_rows,
    mid_proj,
    pbuf,
    last_proj,
    pace,
    first_pace,
    first_right,
    first_left,
    lift_pieces,
    probe_pieces,
    solver,
    sum_pieces,
    hand,
    handed,
    mass_out,
    mass_in,
    load_sem,
    fs_send,
    fs_recv,
    fg_send,
    fg_recv,
    ls_send,
    ls_recv,
    lg_send,
    lg_recv,
    fp_send,
    fp_recv,
    mp_send,
    mp_recv,
    lp_send,
    lp_recv,
    chip_send,
    chip_recv,
    clear,
):
    me = lax.axis_index("tm")
    span = lax.axis_index("state")
    frames = symbols.shape[0]
    rank, cells = right.shape
    share = rank // tiles
    states = cells * tiles
    pairs = [(t, s) for s in range(frames) for t in range(s + 1, frames)]
    sums = [(t, s) for s in range(frames) for t in range(s + 1, frames + 1)]
    base = len(pairs) * rank
    width = last_full.shape[1]
    first_width = first_full.shape[1]
    skip = (frames - 1) * rank // 128 * 128
    peers = [lax.rem(me + k, tiles) for k in range(tiles)]
    half = rank + 32

    loads = [
        pltpu.make_async_copy(src, dst, load_sem.at[i])
        for i, (src, dst) in enumerate(
            (
                (emission_hbm, emission),
                (decay_hbm, decay),
                (left_hbm.at[0], left),
                (right_hbm.at[0], right),
                (initial_hbm, entry),
            )
        )
    ]
    for load in loads:
        load.start()

    barrier = pltpu.get_barrier_semaphore()

    @pl.when(span < LAST)
    def _():
        for k in range(tiles):
            pl.semaphore_signal(barrier, inc=1, device_id={"tm": peers[k], "state": LAST})

    @pl.when(span == LAST)
    def _():
        for k in range(1, tiles):
            pl.semaphore_signal(barrier, inc=1, device_id={"tm": peers[k], "state": LAST})
        for k in range(tiles):
            pl.semaphore_signal(barrier, inc=1, device_id={"tm": peers[k], "state": 0})

    def remote(src, dst, send, recv, tile, state):
        return pltpu.make_async_remote_copy(
            src, dst, send, recv, device_id={"tm": tile, "state": state}
        )

    def first_scatter(k):
        return remote(
            first_pieces.at[peers[k]], first_parts.at[k], fs_send, fs_recv, peers[k], LAST
        )

    def first_project(k):
        return remote(first_row, first_proj.at[k], fp_send, fp_recv, peers[k], LAST)

    def first_gather(k):
        return remote(first_own, first_all.at[me], fg_send, fg_recv, peers[k], LAST)

    def mid_project(k):
        return remote(mid_rows, mid_proj.at[k - 1], mp_send, mp_recv, peers[k], LAST)

    def last_scatter(k):
        return remote(
            last_pieces.at[peers[k]], last_parts.at[k - 1], ls_send, ls_recv, peers[k], LAST
        )

    def last_gather(k):
        return remote(last_own, last_all.at[me], lg_send, lg_recv, peers[k], LAST)

    def last_project(k):
        return remote(pbuf, last_proj.at[k - 1], lp_send, lp_recv, peers[k], LAST)

    def landed(ref, sem):
        pltpu.make_async_copy(ref, ref, sem).wait()

    def give(i):
        src, dst, state = (
            (right, first_right, LAST),
            (pace, first_pace, LAST),
            (hand, handed, 0),
            (mass_out, mass_in, 0),
            (left, first_left, LAST),
        )[i]
        return remote(src, dst, chip_send.at[i], chip_recv.at[i], me, state)

    others = pl.ds(0, tiles - 1)

    row_id = lax.broadcasted_iota(jnp.int32, (ROWS, emission.shape[1]), 0)
    column_id = lax.broadcasted_iota(jnp.int32, (ROWS, emission.shape[1]), 1)
    wanted = jnp.full(row_id.shape, -1, jnp.int32)
    for t in range(frames):
        wanted = jnp.where(row_id == t, symbols[t], wanted)
    onehot = jnp.where(wanted == column_id, 1.0, 0.0).astype(BF16)
    for load in loads:
        load.wait()
    emitted = sum(
        lax.dot_general(onehot, piece, (ALONG, ((), ())), preferred_element_type=F32)
        for piece in split(emission[...])
    )
    emit = [emitted[t : t + 1] for t in range(frames)]
    grow = [emit[t] * decay[...] for t in range(frames)]
    scaled = left[...] * (1.0 / states)
    scaled_pieces = split(scaled)
    for t in range(frames):
        pace[t : t + 1] = emit[t]
        pace[frames + t : frames + t + 1] = grow[t]

    def filled(rows):
        return jnp.concatenate(rows + [jnp.zeros_like(rows[0])] * (ROWS - len(rows)), axis=0)

    def projections(row):
        rows = [row]
        for t in range(frames):
            row = row * grow[t]
            rows.append(row)
        reached = filled(rows)
        pbuf[:, :rank] = dot2(reached, scaled_pieces, ALONG)
        pbuf[:, rank:half] = jnp.broadcast_to(
            jnp.sum(reached, axis=1, keepdims=True), (ROWS, half - rank)
        )

    def couplings():
        reach = {}
        for s in range(frames):
            weight = emit[s]
            reach[s + 1, s] = weight
            for t in range(s + 1, frames):
                weight = weight * grow[t]
                reach[t + 1, s] = weight
        for i, pair in enumerate(pairs):
            side[i * rank : (i + 1) * rank] = reach[pair] * scaled
        side[base:] = jnp.zeros((width - base, cells), F32)
        for i, pair in enumerate(sums):
            side[base + i : base + i + 1] = reach[pair]
        return dot2(right[...], split(side[...]), ALONG)

    def solve(mix, full, origin=0, start=0):
        mix_row = lax.broadcasted_iota(jnp.int32, mix.shape, 0)
        mix = jnp.where(mix_row < frames, mix, 0.0)
        for s in range(start, frames - 1):
            for i, (t, u) in enumerate(pairs):
                if u == s:
                    matrix = split(full[:, i * rank - origin : (i + 1) * rank - origin])
                    term = dot2(mix, matrix, ACROSS)[s : s + 1]
                    mix = mix + jnp.where(mix_row == t, term, 0.0)
        return mix

    def advance(belief, emits, grows, lifted):
        kept = []
        for t in range(frames):
            belief = grows[t] * belief + emits[t] * lifted[t : t + 1]
            kept.append(belief)
        return kept

    def write(kept, mass):
        lane = lax.broadcasted_iota(jnp.int32, (1, 128), 1)
        levels = jnp.ones(lane.shape, F32)
        for t in range(frames):
            packed[t : t + 1] = kept[t] * (states / mass[t + 1])
            levels = jnp.where(lane == t, mass[t + 1] / mass[t], levels)
        packed[frames : frames + 1, :128] = jnp.log(levels)

    coupling = couplings()

    @pl.when(span < LAST)
    def _():
        for j in range(tiles):
            first_pieces[j] = coupling[j * share : (j + 1) * share, skip : skip + first_width]
        row = entry[...]
        first_row[:, :rank] = dot2(filled([row]), scaled_pieces, ALONG)[:1]
        first_row[:, rank:] = jnp.broadcast_to(
            jnp.sum(row, axis=1, keepdims=True), (1, first_row.shape[1] - rank)
        )
        pl.semaphore_wait(barrier, tiles)
        for k in reversed(range(tiles)):
            first_project(k).start()
        for k in reversed(range(tiles)):
            first_scatter(k).start()
        for i in (0, 1, 4):
            give(i).start()
        landed(first_pieces, fs_send)
        pl.semaphore_signal(clear, inc=1, device_id={"tm": me, "state": LAST})
        landed(first_proj, fp_send)
        for i in (0, 1, 4):
            give(i).wait_send()
        give(2).wait_recv()
        kept = [handed[t : t + 1] for t in range(frames)]
        mass = [handed[frames : frames + 1, :1]]
        give(3).wait_recv()
        mass += [mass_in[t : t + 1, half : half + 1] for t in range(frames - 1)]
        mass += [mass_in[0:1, rank : rank + 1]]
        write(kept, mass)

    @pl.when(span == LAST)
    def _():
        for j in range(tiles):
            last_pieces[j] = coupling[j * share : (j + 1) * share]
        pl.semaphore_wait(barrier, 2 * tiles - 1)
        pl.semaphore_wait(clear, 1)
        for k in range(1, tiles):
            last_scatter(k).start()
        for i in (0, 1, 4):
            give(i).wait_recv()
        for i, piece in enumerate(split(first_right[...])):
            lift_pieces[i] = piece
        for i, piece in enumerate(split(first_left[...] * (1.0 / states))):
            probe_pieces[i] = piece
        emits = [first_pace[t : t + 1] for t in range(frames)]
        grows = [first_pace[frames + t : frames + t + 1] for t in range(frames)]
        landed(first_parts, fs_recv)
        total = first_parts[0]
        for k in range(1, tiles):
            total = total + first_parts[k]
        first_own[...] = total
        for k in range(1, tiles):
            first_gather(k).start()
        first_all[me] = total
        landed(first_proj, fp_recv)
        opening = first_proj[0]
        for k in range(1, tiles):
            opening = opening + first_proj[k]
        mix_first = jnp.broadcast_to(opening[:, :rank], (ROWS, rank))
        lifted = dot2(mix_first, (lift_pieces[0], lift_pieces[1]), ACROSS)
        second = grows[0] * entry[...] + emits[0] * lifted[:1]
        rows = [second]
        for t in range(1, frames - 1):
            rows.append(rows[-1] * grows[t])
        mid_rows[:, :rank] = dot2(filled(rows), (probe_pieces[0], probe_pieces[1]), ALONG)[
            :frames
        ]
        mid_rows[:, rank:] = jnp.zeros((frames, mid_rows.shape[1] - rank), F32)
        for k in range(1, tiles):
            mid_project(k).start()
        landed(last_parts, ls_recv)
        total = last_pieces[me]
        for k in range(1, tiles):
            total = total + last_parts[k - 1]
        last_own[...] = total
        for k in range(1, tiles):
            last_gather(k).start()
        last_all[me] = total

        landed(mid_proj, mp_recv)
        later = mid_rows[...]
        for k in range(1, tiles):
            later = later + mid_proj[k - 1]
        mix = jnp.concatenate(
            [opening[:, :rank], later[: frames - 1, :rank]]
            + [jnp.zeros((1, rank), F32)] * (ROWS - frames),
            axis=0,
        )
        landed(first_all.at[others], fg_recv)
        for j in range(tiles):
            first_full[j * share : (j + 1) * share] = first_all[j]
        mix = solve(mix, first_full, skip, 1)
        lifted = dot2(mix, (lift_pieces[0], lift_pieces[1]), ACROSS)
        kept = [second]
        for t in range(1, frames):
            kept.append(grows[t] * kept[-1] + emits[t] * lifted[t : t + 1])
        belief = kept[-1]
        projections(belief)
        partial = jnp.concatenate(
            kept[:-1] + [jnp.zeros((ROWS + 1 - frames, cells), F32)], axis=0
        )
        pbuf[:, half:] = jnp.broadcast_to(
            jnp.sum(partial, axis=1, keepdims=True), (ROWS, pbuf.shape[1] - half)
        )
        for k in range(1, tiles):
            last_project(k).start()
        for t in range(frames):
            hand[t : t + 1] = kept[t]
        hand[frames : frames + 1] = jnp.broadcast_to(opening[:, rank : rank + 1], (1, cells))
        give(2).start()

        landed(last_all.at[others], lg_recv)
        for j in range(tiles):
            last_full[j * share : (j + 1) * share] = last_all[j]
        direct = {
            pair: last_full[:, i * rank : (i + 1) * rank] for i, pair in enumerate(pairs)
        }
        direct_pieces = {pair: split(direct[pair]) for pair in pairs}
        composed = {}
        for reach in range(1, frames):
            for t, u in pairs:
                if t - u == reach:
                    composed[t, u] = direct[t, u]
                    for v in range(u + 1, t):
                        composed[t, u] = composed[t, u] + dot2(
                            composed[v, u], direct_pieces[t, v], ACROSS
                        )
        for i, pair in enumerate(pairs):
            for j, piece in enumerate(split(composed[pair])):
                solver[2 * i + j] = piece
        for j, piece in enumerate(split(right[...])):
            lift_pieces[j] = piece
        for j, piece in enumerate(split(last_full[:, base:])):
            sum_pieces[j] = piece
        projected = pbuf[...]
        landed(last_proj, lp_recv)
        for k in range(1, tiles):
            projected = projected + last_proj[k - 1]
        mass_out[...] = projected
        give(3).start()
        entering = projected[:, :rank]
        mix_row = lax.broadcasted_iota(jnp.int32, entering.shape, 0)
        entering = jnp.where(mix_row < frames, entering, 0.0)
        mix = entering
        for i, (t, u) in enumerate(pairs):
            term = dot2(entering, (solver[2 * i], solver[2 * i + 1]), ACROSS)[u : u + 1]
            mix = mix + jnp.where(mix_row == t, term, 0.0)
        lifted = dot2(mix, (lift_pieces[0], lift_pieces[1]), ACROSS)
        kept = advance(belief, emit, grow, lifted)
        parts = dot2(mix, (sum_pieces[0], sum_pieces[1]), ACROSS)
        part_row = lax.broadcasted_iota(jnp.int32, parts.shape, 0)
        part_column = lax.broadcasted_iota(jnp.int32, parts.shape, 1)
        mass = [projected[0:1, rank : rank + 1]]
        for t in range(1, frames + 1):
            hit = jnp.zeros(parts.shape, jnp.bool_)
            for i, (u, s) in enumerate(sums):
                if u == t:
                    hit = hit | ((part_row == s) & (part_column == i))
            mass.append(
                projected[t : t + 1, rank : rank + 1]
                + jnp.sum(jnp.where(hit, parts, 0.0), keepdims=True)
            )
        write(kept, mass)
        landed(last_parts, ls_send)
        landed(first_all.at[others], fg_send)
        landed(mid_proj, mp_send)
        landed(last_all.at[others], lg_send)
        landed(last_proj, lp_send)
        give(2).wait_send()
        give(3).wait_send()


def unpack(packed, beliefs_out, logs_out):
    frames = beliefs_out.shape[0]
    beliefs_out[...] = packed[:frames]
    logs_out[...] = packed[frames, :frames]


def solution(mesh):
    tiles = mesh.shape["tm"]
    assert mesh.shape["state"] == LAST + 1

    def per_device(symbols, emission, decay, left_factor, right_factor, initial):
        frames = symbols.shape[0]
        rank, cells = left_factor.shape[1:]
        pair_count = frames * (frames - 1) // 2
        sum_count = frames * (frames + 1) // 2
        base = pair_count * rank
        first_width = -(-base // 128) * 128 - (frames - 1) * rank // 128 * 128
        width = -(-(pair_count * rank + sum_count) // 128) * 128
        share = rank // tiles
        vmem, dma = pltpu.VMEM, pltpu.SemaphoreType.DMA
        others = tiles - 1
        packed = pl.pallas_call(
            functools.partial(kernel, tiles),
            out_shape=vmem((ROWS, cells), F32),
            in_specs=[pl.BlockSpec(memory_space=pltpu.SMEM)]
            + [pl.BlockSpec(memory_space=pltpu.HBM)] * 5,
            out_specs=pl.BlockSpec(memory_space=vmem),
            scratch_shapes=[
                vmem(emission.shape, F32),
                vmem(decay.shape, F32),
                vmem((rank, cells), F32),
                vmem((rank, cells), F32),
                vmem((1, cells), F32),
                vmem((width, cells), F32),
                vmem((tiles, share, first_width), F32),
                vmem((tiles, share, first_width), F32),
                vmem((share, first_width), F32),
                vmem((tiles, share, first_width), F32),
                vmem((rank, first_width), F32),
                vmem((tiles, share, width), F32),
                vmem((others, share, width), F32),
                vmem((share, width), F32),
                vmem((tiles, share, width), F32),
                vmem((rank, width), F32),
                vmem((1, 128), F32),
                vmem((tiles, 1, 128), F32),
                vmem((frames, 128), F32),
                vmem((others, frames, 128), F32),
                vmem((ROWS, 128), F32),
                vmem((others, ROWS, 128), F32),
                vmem((2 * frames, cells), F32),
                vmem((2 * frames, cells), F32),
                vmem((rank, cells), F32),
                vmem((rank, cells), F32),
                vmem((2, rank, cells), BF16),
                vmem((2, rank, cells), BF16),
                vmem((2 * pair_count, rank, rank), BF16),
                vmem((2, rank, width - base), BF16),
                vmem((ROWS, cells), F32),
                vmem((ROWS, cells), F32),
                vmem((ROWS, 128), F32),
                vmem((ROWS, 128), F32),
                dma((5,)),
                *[dma(())] * 14,
                dma((5,)),
                dma((5,)),
                pltpu.SemaphoreType.REGULAR,
            ],
            compiler_params=pltpu.CompilerParams(collective_id=0, has_side_effects=True),
        )(symbols, emission, decay, left_factor, right_factor, initial.reshape(1, cells))
        return pl.pallas_call(
            unpack,
            out_shape=(
                jax.ShapeDtypeStruct((frames, cells), F32),
                jax.ShapeDtypeStruct((frames,), F32),
            ),
            in_specs=[pl.BlockSpec(memory_space=vmem)],
            out_specs=(pl.BlockSpec(memory_space=vmem),) * 2,
            compiler_params=pltpu.CompilerParams(vmem_limit_bytes=16 * 2**20),
        )(packed)

    return jax.shard_map(
        per_device,
        mesh=mesh,
        in_specs=(
            P("state"),
            P("tm", None),
            P("state", "tm"),
            P("state", None, "tm"),
            P("state", None, "tm"),
            P("tm"),
        ),
        out_specs=(P("state", "tm"), P("state")),
        check_vma=False,
    )
```

```python
import functools

import jax
import jax.numpy as jnp
from jax import lax
from jax.experimental import pallas as pl
from jax.experimental.pallas import tpu as pltpu
from jax.sharding import PartitionSpec as P

F32 = jnp.float32
BF16 = jnp.bfloat16
ROWS = 8


def split(x):
    hi = x.astype(BF16)
    return hi, (x - hi.astype(F32)).astype(BF16)


def stacked(x):
    hi = x.astype(BF16).astype(F32)
    return jnp.concatenate([hi, x - hi], axis=0).astype(BF16)


def dot2(x, pieces, dims):
    both = stacked(x)
    total = sum(
        lax.dot_general(both, piece, (dims, ((), ())), preferred_element_type=F32)
        for piece in pieces
    )
    return total[: x.shape[0]] + total[x.shape[0] :]


ALONG = ((1,), (1,))
ACROSS = ((1,), (0,))
LAST = 1


def kernel(
    tiles,
    symbols,
    emission_hbm,
    decay_hbm,
    left_hbm,
    right_hbm,
    initial_hbm,
    packed,
    emission,
    decay,
    left,
    right,
    entry,
    side,
    first_pieces,
    first_parts,
    first_own,
    first_all,
    first_full,
    last_pieces,
    last_parts,
    last_own,
    last_all,
    last_full,
    first_row,
    first_proj,
    mid_rows,
    mid_proj,
    pbuf,
    last_proj,
    pace,
    first_pace,
    first_right,
    first_left,
    lift_pieces,
    probe_pieces,
    solver,
    sum_pieces,
    hand,
    handed,
    mass_out,
    mass_in,
    load_sem,
    fs_send,
    fs_recv,
    fg_send,
    fg_recv,
    ls_send,
    ls_recv,
    lg_send,
    lg_recv,
    fp_send,
    fp_recv,
    mp_send,
    mp_recv,
    lp_send,
    lp_recv,
    chip_send,
    chip_recv,
    clear,
):
    me = lax.axis_index("tm")
    span = lax.axis_index("state")
    frames = symbols.shape[0]
    rank, cells = right.shape
    share = rank // tiles
    states = cells * tiles
    pairs = [(t, s) for s in range(frames) for t in range(s + 1, frames)]
    sums = [(t, s) for s in range(frames) for t in range(s + 1, frames + 1)]
    base = len(pairs) * rank
    width = last_full.shape[1]
    first_width = first_full.shape[1]
    skip = (frames - 1) * rank // 128 * 128
    peers = [lax.rem(me + k, tiles) for k in range(tiles)]
    half = rank + 32

    loads = [
        pltpu.make_async_copy(src, dst, load_sem.at[i])
        for i, (src, dst) in enumerate(
            (
                (emission_hbm, emission),
                (decay_hbm, decay),
                (left_hbm.at[0], left),
                (right_hbm.at[0], right),
                (initial_hbm, entry),
            )
        )
    ]
    for load in loads:
        load.start()

    barrier = pltpu.get_barrier_semaphore()

    @pl.when(span < LAST)
    def _():
        for k in range(tiles):
            pl.semaphore_signal(barrier, inc=1, device_id={"tm": peers[k], "state": LAST})

    @pl.when(span == LAST)
    def _():
        for k in range(1, tiles):
            pl.semaphore_signal(barrier, inc=1, device_id={"tm": peers[k], "state": LAST})
        for k in range(tiles):
            pl.semaphore_signal(barrier, inc=1, device_id={"tm": peers[k], "state": 0})

    def remote(src, dst, send, recv, tile, state):
        return pltpu.make_async_remote_copy(
            src, dst, send, recv, device_id={"tm": tile, "state": state}
        )

    def first_scatter(k):
        return remote(
            first_pieces.at[peers[k]], first_parts.at[k], fs_send, fs_recv, peers[k], LAST
        )

    def first_project(k):
        return remote(first_row, first_proj.at[k], fp_send, fp_recv, peers[k], LAST)

    def first_gather(k):
        return remote(first_own, first_all.at[me], fg_send, fg_recv, peers[k], LAST)

    def mid_project(k):
        return remote(mid_rows, mid_proj.at[k - 1], mp_send, mp_recv, peers[k], LAST)

    def last_scatter(k):
        return remote(
            last_pieces.at[peers[k]], last_parts.at[k - 1], ls_send, ls_recv, peers[k], LAST
        )

    def last_gather(k):
        return remote(last_own, last_all.at[me], lg_send, lg_recv, peers[k], LAST)

    def last_project(k):
        return remote(pbuf, last_proj.at[k - 1], lp_send, lp_recv, peers[k], LAST)

    def landed(ref, sem):
        pltpu.make_async_copy(ref, ref, sem).wait()

    def give(i):
        src, dst, state = (
            (right, first_right, LAST),
            (pace, first_pace, LAST),
            (hand, handed, 0),
            (mass_out, mass_in, 0),
            (left, first_left, LAST),
        )[i]
        return remote(src, dst, chip_send.at[i], chip_recv.at[i], me, state)

    others = pl.ds(0, tiles - 1)

    row_id = lax.broadcasted_iota(jnp.int32, (ROWS, emission.shape[1]), 0)
    column_id = lax.broadcasted_iota(jnp.int32, (ROWS, emission.shape[1]), 1)
    wanted = jnp.full(row_id.shape, -1, jnp.int32)
    for t in range(frames):
        wanted = jnp.where(row_id == t, symbols[t], wanted)
    onehot = jnp.where(wanted == column_id, 1.0, 0.0).astype(BF16)
    for load in loads:
        load.wait()
    emitted = sum(
        lax.dot_general(onehot, piece, (ALONG, ((), ())), preferred_element_type=F32)
        for piece in split(emission[...])
    )
    emit = [emitted[t : t + 1] for t in range(frames)]
    grow = [emit[t] * decay[...] for t in range(frames)]
    scaled = left[...] * (1.0 / states)
    scaled_pieces = split(scaled)
    for t in range(frames):
        pace[t : t + 1] = emit[t]
        pace[frames + t : frames + t + 1] = grow[t]

    def filled(rows):
        return jnp.concatenate(rows + [jnp.zeros_like(rows[0])] * (ROWS - len(rows)), axis=0)

    def projections(row):
        rows = [row]
        for t in range(frames):
            row = row * grow[t]
            rows.append(row)
        reached = filled(rows)
        pbuf[:, :rank] = dot2(reached, scaled_pieces, ALONG)
        pbuf[:, rank:half] = jnp.broadcast_to(
            jnp.sum(reached, axis=1, keepdims=True), (ROWS, half - rank)
        )

    def couplings():
        reach = {}
        for s in range(frames):
            weight = emit[s]
            reach[s + 1, s] = weight
            for t in range(s + 1, frames):
                weight = weight * grow[t]
                reach[t + 1, s] = weight
        for i, pair in enumerate(pairs):
            side[i * rank : (i + 1) * rank] = reach[pair] * scaled
        side[base:] = jnp.zeros((width - base, cells), F32)
        for i, pair in enumerate(sums):
            side[base + i : base + i + 1] = reach[pair]
        return dot2(right[...], split(side[...]), ALONG)

    def solve(mix, full, origin=0, start=0):
        mix_row = lax.broadcasted_iota(jnp.int32, mix.shape, 0)
        mix = jnp.where(mix_row < frames, mix, 0.0)
        for s in range(start, frames - 1):
            for i, (t, u) in enumerate(pairs):
                if u == s:
                    matrix = split(full[:, i * rank - origin : (i + 1) * rank - origin])
                    term = dot2(mix, matrix, ACROSS)[s : s + 1]
                    mix = mix + jnp.where(mix_row == t, term, 0.0)
        return mix

    def advance(belief, emits, grows, lifted):
        kept = []
        for t in range(frames):
            belief = grows[t] * belief + emits[t] * lifted[t : t + 1]
            kept.append(belief)
        return kept

    def write(kept, mass):
        lane = lax.broadcasted_iota(jnp.int32, (1, 128), 1)
        levels = jnp.ones(lane.shape, F32)
        for t in range(frames):
            packed[t : t + 1] = kept[t] * (states / mass[t + 1])
            levels = jnp.where(lane == t, mass[t + 1] / mass[t], levels)
        packed[frames : frames + 1, :128] = jnp.log(levels)

    coupling = couplings()

    @pl.when(span < LAST)
    def _():
        for j in range(tiles):
            first_pieces[j] = coupling[j * share : (j + 1) * share, skip : skip + first_width]
        row = entry[...]
        first_row[:, :rank] = dot2(filled([row]), scaled_pieces, ALONG)[:1]
        first_row[:, rank:] = jnp.broadcast_to(
            jnp.sum(row, axis=1, keepdims=True), (1, first_row.shape[1] - rank)
        )
        pl.semaphore_wait(barrier, tiles)
        for k in reversed(range(tiles)):
            first_project(k).start()
        for k in reversed(range(tiles)):
            first_scatter(k).start()
        for i in (0, 1, 4):
            give(i).start()
        landed(first_pieces, fs_send)
        pl.semaphore_signal(clear, inc=1, device_id={"tm": me, "state": LAST})
        landed(first_proj, fp_send)
        for i in (0, 1, 4):
            give(i).wait_send()
        give(2).wait_recv()
        kept = [handed[t : t + 1] for t in range(frames)]
        mass = [handed[frames : frames + 1, :1]]
        give(3).wait_recv()
        mass += [mass_in[t : t + 1, half : half + 1] for t in range(frames - 1)]
        mass += [mass_in[0:1, rank : rank + 1]]
        write(kept, mass)

    @pl.when(span == LAST)
    def _():
        for j in range(tiles):
            last_pieces[j] = coupling[j * share : (j + 1) * share]
        pl.semaphore_wait(barrier, 2 * tiles - 1)
        pl.semaphore_wait(clear, 1)
        for k in range(1, tiles):
            last_scatter(k).start()
        for i in (0, 1, 4):
            give(i).wait_recv()
        for i, piece in enumerate(split(first_right[...])):
            lift_pieces[i] = piece
        for i, piece in enumerate(split(first_left[...] * (1.0 / states))):
            probe_pieces[i] = piece
        emits = [first_pace[t : t + 1] for t in range(frames)]
        grows = [first_pace[frames + t : frames + t + 1] for t in range(frames)]
        landed(first_proj, fp_recv)
        opening = first_proj[0]
        for k in range(1, tiles):
            opening = opening + first_proj[k]
        mix_first = jnp.broadcast_to(opening[:, :rank], (ROWS, rank))
        lifted = dot2(mix_first, (lift_pieces[0], lift_pieces[1]), ACROSS)
        second = grows[0] * entry[...] + emits[0] * lifted[:1]
        rows = [second]
        for t in range(1, frames - 1):
            rows.append(rows[-1] * grows[t])
        mid_rows[:, :rank] = dot2(filled(rows), (probe_pieces[0], probe_pieces[1]), ALONG)[
            :frames
        ]
        mid_rows[:, rank:] = jnp.zeros((frames, mid_rows.shape[1] - rank), F32)
        for k in range(1, tiles):
            mid_project(k).start()
        landed(first_parts, fs_recv)
        total = first_parts[0]
        for k in range(1, tiles):
            total = total + first_parts[k]
        first_own[...] = total
        for k in range(1, tiles):
            first_gather(k).start()
        first_all[me] = total
        landed(last_parts, ls_recv)
        total = last_pieces[me]
        for k in range(1, tiles):
            total = total + last_parts[k - 1]
        last_own[...] = total
        for k in range(1, tiles):
            last_gather(k).start()
        last_all[me] = total

        landed(mid_proj, mp_recv)
        later = mid_rows[...]
        for k in range(1, tiles):
            later = later + mid_proj[k - 1]
        mix = jnp.concatenate(
            [opening[:, :rank], later[: frames - 1, :rank]]
            + [jnp.zeros((1, rank), F32)] * (ROWS - frames),
            axis=0,
        )
        landed(first_all.at[others], fg_recv)
        for j in range(tiles):
            first_full[j * share : (j + 1) * share] = first_all[j]
        mix = solve(mix, first_full, skip, 1)
        lifted = dot2(mix, (lift_pieces[0], lift_pieces[1]), ACROSS)
        kept = [second]
        for t in range(1, frames):
            kept.append(grows[t] * kept[-1] + emits[t] * lifted[t : t + 1])
        belief = kept[-1]
        projections(belief)
        partial = jnp.concatenate(
            kept[:-1] + [jnp.zeros((ROWS + 1 - frames, cells), F32)], axis=0
        )
        pbuf[:, half:] = jnp.broadcast_to(
            jnp.sum(partial, axis=1, keepdims=True), (ROWS, pbuf.shape[1] - half)
        )
        for k in range(1, tiles):
            last_project(k).start()
        for t in range(frames):
            hand[t : t + 1] = kept[t]
        hand[frames : frames + 1] = jnp.broadcast_to(opening[:, rank : rank + 1], (1, cells))
        give(2).start()

        landed(last_all.at[others], lg_recv)
        for j in range(tiles):
            last_full[j * share : (j + 1) * share] = last_all[j]
        direct = {
            pair: last_full[:, i * rank : (i + 1) * rank] for i, pair in enumerate(pairs)
        }
        direct_pieces = {pair: split(direct[pair]) for pair in pairs}
        composed = {}
        for reach in range(1, frames):
            for t, u in pairs:
                if t - u == reach:
                    composed[t, u] = direct[t, u]
                    for v in range(u + 1, t):
                        composed[t, u] = composed[t, u] + dot2(
                            composed[v, u], direct_pieces[t, v], ACROSS
                        )
        for i, pair in enumerate(pairs):
            for j, piece in enumerate(split(composed[pair])):
                solver[2 * i + j] = piece
        for j, piece in enumerate(split(right[...])):
            lift_pieces[j] = piece
        for j, piece in enumerate(split(last_full[:, base:])):
            sum_pieces[j] = piece
        projected = pbuf[...]
        landed(last_proj, lp_recv)
        for k in range(1, tiles):
            projected = projected + last_proj[k - 1]
        mass_out[...] = projected
        give(3).start()
        entering = projected[:, :rank]
        mix_row = lax.broadcasted_iota(jnp.int32, entering.shape, 0)
        entering = jnp.where(mix_row < frames, entering, 0.0)
        mix = entering
        for i, (t, u) in enumerate(pairs):
            term = dot2(entering, (solver[2 * i], solver[2 * i + 1]), ACROSS)[u : u + 1]
            mix = mix + jnp.where(mix_row == t, term, 0.0)
        lifted = dot2(mix, (lift_pieces[0], lift_pieces[1]), ACROSS)
        kept = advance(belief, emit, grow, lifted)
        parts = dot2(mix, (sum_pieces[0], sum_pieces[1]), ACROSS)
        part_row = lax.broadcasted_iota(jnp.int32, parts.shape, 0)
        part_column = lax.broadcasted_iota(jnp.int32, parts.shape, 1)
        mass = [projected[0:1, rank : rank + 1]]
        for t in range(1, frames + 1):
            hit = jnp.zeros(parts.shape, jnp.bool_)
            for i, (u, s) in enumerate(sums):
                if u == t:
                    hit = hit | ((part_row == s) & (part_column == i))
            mass.append(
                projected[t : t + 1, rank : rank + 1]
                + jnp.sum(jnp.where(hit, parts, 0.0), keepdims=True)
            )
        write(kept, mass)
        landed(last_parts, ls_send)
        landed(first_all.at[others], fg_send)
        landed(mid_proj, mp_send)
        landed(last_all.at[others], lg_send)
        landed(last_proj, lp_send)
        give(2).wait_send()
        give(3).wait_send()


def unpack(packed, beliefs_out, logs_out):
    frames = beliefs_out.shape[0]
    beliefs_out[...] = packed[:frames]
    logs_out[...] = packed[frames, :frames]


def solution(mesh):
    tiles = mesh.shape["tm"]
    assert mesh.shape["state"] == LAST + 1

    def per_device(symbols, emission, decay, left_factor, right_factor, initial):
        frames = symbols.shape[0]
        rank, cells = left_factor.shape[1:]
        pair_count = frames * (frames - 1) // 2
        sum_count = frames * (frames + 1) // 2
        base = pair_count * rank
        first_width = -(-base // 128) * 128 - (frames - 1) * rank // 128 * 128
        width = -(-(pair_count * rank + sum_count) // 128) * 128
        share = rank // tiles
        vmem, dma = pltpu.VMEM, pltpu.SemaphoreType.DMA
        others = tiles - 1
        packed = pl.pallas_call(
            functools.partial(kernel, tiles),
            out_shape=vmem((ROWS, cells), F32),
            in_specs=[pl.BlockSpec(memory_space=pltpu.SMEM)]
            + [pl.BlockSpec(memory_space=pltpu.HBM)] * 5,
            out_specs=pl.BlockSpec(memory_space=vmem),
            scratch_shapes=[
                vmem(emission.shape, F32),
                vmem(decay.shape, F32),
                vmem((rank, cells), F32),
                vmem((rank, cells), F32),
                vmem((1, cells), F32),
                vmem((width, cells), F32),
                vmem((tiles, share, first_width), F32),
                vmem((tiles, share, first_width), F32),
                vmem((share, first_width), F32),
                vmem((tiles, share, first_width), F32),
                vmem((rank, first_width), F32),
                vmem((tiles, share, width), F32),
                vmem((others, share, width), F32),
                vmem((share, width), F32),
                vmem((tiles, share, width), F32),
                vmem((rank, width), F32),
                vmem((1, 128), F32),
                vmem((tiles, 1, 128), F32),
                vmem((frames, 128), F32),
                vmem((others, frames, 128), F32),
                vmem((ROWS, 128), F32),
                vmem((others, ROWS, 128), F32),
                vmem((2 * frames, cells), F32),
                vmem((2 * frames, cells), F32),
                vmem((rank, cells), F32),
                vmem((rank, cells), F32),
                vmem((2, rank, cells), BF16),
                vmem((2, rank, cells), BF16),
                vmem((2 * pair_count, rank, rank), BF16),
                vmem((2, rank, width - base), BF16),
                vmem((ROWS, cells), F32),
                vmem((ROWS, cells), F32),
                vmem((ROWS, 128), F32),
                vmem((ROWS, 128), F32),
                dma((5,)),
                *[dma(())] * 14,
                dma((5,)),
                dma((5,)),
                pltpu.SemaphoreType.REGULAR,
            ],
            compiler_params=pltpu.CompilerParams(collective_id=0, has_side_effects=True),
        )(symbols, emission, decay, left_factor, right_factor, initial.reshape(1, cells))
        return pl.pallas_call(
            unpack,
            out_shape=(
                jax.ShapeDtypeStruct((frames, cells), F32),
                jax.ShapeDtypeStruct((frames,), F32),
            ),
            in_specs=[pl.BlockSpec(memory_space=vmem)],
            out_specs=(pl.BlockSpec(memory_space=vmem),) * 2,
            compiler_params=pltpu.CompilerParams(vmem_limit_bytes=16 * 2**20),
        )(packed)

    return jax.shard_map(
        per_device,
        mesh=mesh,
        in_specs=(
            P("state"),
            P("tm", None),
            P("state", "tm"),
            P("state", None, "tm"),
            P("state", None, "tm"),
            P("tm"),
        ),
        out_specs=(P("state", "tm"), P("state")),
        check_vma=False,
    )
```
